128 devices in a mesh: fsdp: 32 (over z_hi, y, x), tp: 4 (over z_lo, core).
Axes of the slice: x: 4, y: 4, z: 4 (z_hi: 2, z_lo: 2; z = z_hi * 2 + z_lo), core: 2. Of those that a mesh axis runs over, the one named last changes fastest.
Arguments:
- weights: bfloat16 [8192, 16384], P('fsdp', 'tp')
- owner_map: int32 [128, 256], P(('fsdp', 'tp')), may hold values from 0 to 127, as said below
Outputs:
- served_tiles: bfloat16 [32768, 32, 128], P(('fsdp', 'tp'))
- served_scales: float32 [32768, 128], P(('fsdp', 'tp'))
The draws below stay inside these ranges and needn't reach their ends.
Inputs may be any that keep to these rules, and one draw needn't show every extreme that they name: `owner_map`: each source device's row names every destination exactly 2 times.
All inputs are finite; a program needn't handle non-finite values. Where the reference program divides by a largest or mean magnitude, that divisor is 1e-20 or more.
Results may differ from the reference program's by a relative error of at most 0.0055.
Values may be sent and summed in bfloat16 or wider, within the bound.
A program may use at most 64 MiB of HBM per device.

```python
import jax
import jax.numpy as jnp
from jax import lax

COLS = 16384
TILE_COLS = 128
ROWS_DEV = 256
FF_WIN = 8192
TILES_DEV = 256
PER_PEER = 2
N_FSDP = 32
N_TP = 4
DEVICES = 128


def draw_weights(key, part):
    first, second, third, fourth = jax.random.split(key, 4)
    blocks = FF_WIN // 32
    block_scale = jnp.exp(jax.random.uniform(first, (blocks, 1), jnp.float32, jnp.log(0.1), jnp.log(10.0)))
    row_scale = jnp.repeat(block_scale, 32, axis=0)
    row_scale = row_scale * jax.random.uniform(second, (FF_WIN, 1), jnp.float32, 0.5, 1.5)
    rising = 1.0 + 2.0 * jnp.arange(FF_WIN, dtype=jnp.float32)[:, None] / FF_WIN
    column_scale = jax.random.uniform(third, (1, COLS), jnp.float32, 0.5, 1.5)
    base = jnp.clip(jax.random.normal(fourth, (FF_WIN, COLS), jnp.float32), -6.0, 6.0)
    return (base * row_scale * rising * column_scale).astype(jnp.bfloat16)


def draw_owner_map(key, part):
    keys = jax.vmap(lambda index: jax.random.fold_in(jax.random.fold_in(key, 77), index))(jnp.arange(DEVICES))
    orders = jax.vmap(lambda one: jax.random.permutation(one, TILES_DEV))(keys)
    return (orders // PER_PEER).astype(jnp.int32)


def setup_inputs(seed: int = 0) -> dict:
    key_of = jax.random.split(jax.random.key(seed), 3)
    weights = draw_weights(jax.random.fold_in(key_of[2], 71), 0)
    owner_map = draw_owner_map(jax.random.fold_in(key_of[2], 71), 0)
    return dict(weights=weights, owner_map=owner_map)


block_rows = 32


def reference(weights, owner_map):
    global_amax = jnp.max(jnp.abs(weights)).astype(jnp.float32)
    row_blocks = ROWS_DEV // block_rows
    col_blocks = COLS // N_TP // TILE_COLS
    tiles = weights.reshape(N_FSDP, row_blocks, block_rows, N_TP, col_blocks, TILE_COLS)
    tiles = tiles.transpose(0, 3, 1, 4, 2, 5).reshape(DEVICES, TILES_DEV, block_rows, TILE_COLS)

    def one_source(item):
        source_tiles, targets = item
        values = source_tiles.astype(jnp.float32)
        clipped = jnp.maximum(jnp.max(jnp.abs(values), axis=1), 1.0)
        factor = 448.0 / clipped
        quantized = (values * factor[:, None, :]).astype(jnp.bfloat16)
        relative = clipped / global_amax
        order = jnp.argsort(targets, stable=True).astype(jnp.int32)
        return quantized[order], relative[order]

    packed, scales = lax.map(one_source, (tiles, owner_map))
    packed = packed.reshape(DEVICES, DEVICES, PER_PEER, block_rows, TILE_COLS).transpose(1, 0, 2, 3, 4)
    scales = scales.reshape(DEVICES, DEVICES, PER_PEER, TILE_COLS).transpose(1, 0, 2, 3)
    served_tiles = packed.reshape(DEVICES * TILES_DEV, block_rows, TILE_COLS)
    served_scales = scales.reshape(DEVICES * TILES_DEV, TILE_COLS)
    return served_tiles, served_scales
```

```python
import random

import jax
import jax.numpy as jnp
from jax import lax
from jax.experimental import pallas as pl
from jax.experimental.pallas import tpu as pltpu
from jax.sharding import PartitionSpec as P

MESH = pl.DeviceIdType.MESH
N = 128
TILES = 256
ROWS = 32
LANES = 128
BLOCKS = 32
F32 = jnp.float32
BF16 = jnp.bfloat16
I32 = jnp.int32


def _hops(m):
    ring = (0, 1, 2, 1)
    return ring[(m >> 2) & 3] + ring[(m >> 4) & 3] + ring[(m >> 6) * 2 + ((m >> 1) & 1)]


def _plane(m):
    return (m >> 6) == 0 and ((m >> 1) & 1) == 0


PRE = 40
_rng = random.Random(3)
_all = list(range(1, N))
_rng.shuffle(_all)
_all.sort(key=lambda m: -_hops(m))
NEAR = [m for m in _all if _hops(m) <= 3 or _plane(m)]
_first = [m for m in _all if _hops(m) == 3][:PRE]
ORDER = _first + [m for m in _all if m not in _first] + [0]
LINE_Z = [2, 64, 66]
LINE_Y = [16, 32, 48]
LINE_X = [1, 4, 5, 8, 9, 12, 13]
CUTS = list(range(0, 120, 8)) + [120, 124, 127]
LINES = len(LINE_X) + len(LINE_Y) + len(LINE_Z)


def _dev(p):
    return (lax.div(p, 4), lax.rem(p, 4))


def _body(w_hbm, map_hbm, out_ref, scale_ref, wv, sbuf, rbuf, table, map_s, pos_v, pos_s,
          peak_out, peak_in, copy_sem, map_sem, pos_sem, send_sem, recv_sem, peak_send, peak_recv, all_sem):
    me = lax.axis_index("fsdp") * 4 + lax.axis_index("tp")
    barrier = pltpu.get_barrier_semaphore()

    def partner(m):
        return jnp.bitwise_xor(me, m)

    map_copy = pltpu.make_async_copy(map_hbm, map_s, map_sem)
    map_copy.start()
    for m in NEAR:
        pl.semaphore_signal(barrier, inc=1, device_id=_dev(partner(m)), device_id_type=MESH)
    w_copies = []
    for c in range(BLOCKS):
        w_copies.append(pltpu.make_async_copy(
            w_hbm.at[:, :, pl.ds(c * LANES, LANES)], wv.at[pl.ds(c * 8, 8)], copy_sem))
        w_copies[-1].start()

    for k, m in enumerate(ORDER):
        table[k] = m

    map_copy.wait()
    lane = lax.broadcasted_iota(I32, (8, LANES), 1)

    def slot(j):
        return lax.rem(j, BLOCKS) * 8 + lax.div(j, BLOCKS)

    def find(i, pos):
        low, high = pos
        for u in range(8):
            up = i * 8 + u
            down = TILES - 1 - up
            high = jnp.where(lane == map_s[0, up], slot(up), high)
            low = jnp.where(lane == map_s[0, down], slot(down), low)
        return low, high

    zero = jnp.zeros((8, LANES), I32)
    low, high = lax.fori_loop(0, TILES // 8, find, (zero, zero))
    pos_v[0] = low
    pos_v[1] = high
    pos_copy = pltpu.make_async_copy(pos_v, pos_s, pos_sem)
    pos_copy.start()

    pltpu.make_async_copy(wv, wv, copy_sem).wait()

    def largest(i, acc):
        x = jnp.abs(wv[pl.ds(i * 8, 8)])
        return jnp.maximum(acc, jnp.max(x.reshape(16, 16, LANES), axis=0))

    peak = lax.fori_loop(0, BLOCKS, largest, jnp.zeros((16, LANES), BF16)).astype(F32)
    peak = jnp.maximum(peak[:8], peak[8:])
    peak_out[0] = peak

    pos_copy.wait()

    def gather(i, _):
        for u in range(4):
            d = i * 4 + u
            for h in range(2):
                sbuf[d, h] = wv[pos_s[h, 0, d]]
        return 0

    lax.fori_loop(0, N // 4, gather, 0)

    def message(k, p, group):
        return pltpu.make_async_remote_copy(
            src_ref=sbuf.at[p], dst_ref=rbuf.at[k], send_sem=send_sem, recv_sem=recv_sem.at[group],
            device_id=_dev(p), device_id_type=MESH)

    def send(group):
        def one(k, _):
            message(k, partner(table[k]), group).start()
            return 0

        lax.fori_loop(CUTS[group], CUTS[group + 1], one, 0)

    def arrivals(group):
        span = pl.ds(CUTS[group], CUTS[group + 1] - CUTS[group])
        return pltpu.make_async_remote_copy(
            src_ref=sbuf.at[span], dst_ref=rbuf.at[span], send_sem=send_sem, recv_sem=recv_sem.at[group],
            device_id=_dev(me), device_id_type=MESH)

    def peaks(stage, line, base):
        copies = [pltpu.make_async_remote_copy(
            src_ref=peak_out.at[stage], dst_ref=peak_in.at[base + i],
            send_sem=peak_send, recv_sem=peak_recv.at[stage],
            device_id=_dev(partner(m)), device_id_type=MESH) for i, m in enumerate(line)]
        for c in copies:
            c.start()

    def fold(stage, line, base, value):
        span = pl.ds(base, len(line))
        pltpu.make_async_remote_copy(
            src_ref=peak_in.at[span], dst_ref=peak_in.at[span], send_sem=peak_send, recv_sem=peak_recv.at[stage],
            device_id=_dev(me), device_id_type=MESH).wait_recv()
        for i in range(len(line)):
            value = jnp.maximum(value, peak_in[base + i])
        return value

    def finish(p, pair):
        x = pair.astype(F32)
        clipped = jnp.maximum(jnp.max(jnp.abs(x), axis=1, keepdims=True), 1.0)
        out_ref[pl.ds(2 * p, 2)] = (x * (448.0 / clipped)).astype(BF16)
        scale_ref[pl.ds(2 * p, 2), :] = clipped.reshape(2, LANES)

    def receive(group):
        arrivals(group).wait_recv()

        def one(k, _):
            finish(partner(table[k]), rbuf[k])
            return 0

        lax.fori_loop(CUTS[group], CUTS[group + 1], one, 0)

    pl.semaphore_wait(barrier, len(NEAR))
    for m in LINE_Z:
        pl.semaphore_signal(all_sem, inc=1, device_id=_dev(partner(m)), device_id_type=MESH)
    peaks(0, LINE_X, 0)
    for g in range(PRE // 8):
        send(g)
    pl.semaphore_wait(all_sem, len(LINE_Z))
    half = max(PRE // 8, 6)
    for g in range(PRE // 8, half):
        send(g)
    peak = fold(0, LINE_X, 0, peak)
    peak_out[1] = peak
    finish(me, sbuf[me])
    peaks(1, LINE_Y, len(LINE_X))
    for g in range(half, 11):
        send(g)
    for g in range(2):
        receive(g)
    peak = fold(1, LINE_Y, len(LINE_X), peak)
    peak_out[2] = peak
    receive(2)
    peaks(2, LINE_Z, len(LINE_X) + len(LINE_Y))
    for g in range(11, len(CUTS) - 1):
        send(g)
    for g in range(3, 12):
        receive(g)
    peak = fold(2, LINE_Z, len(LINE_X) + len(LINE_Y), peak)
    top = jnp.max(peak, keepdims=True)
    for g in range(12, len(CUTS) - 1):
        receive(g)
    scale_ref[...] = scale_ref[...] / top
    every = pl.ds(0, N - 1)
    pltpu.make_async_remote_copy(
        src_ref=sbuf.at[every], dst_ref=rbuf.at[every], send_sem=send_sem, recv_sem=recv_sem.at[0],
        device_id=_dev(me), device_id_type=MESH).wait_send()
    every = pl.ds(0, LINES)
    pltpu.make_async_remote_copy(
        src_ref=peak_in.at[every], dst_ref=peak_in.at[every], send_sem=peak_send, recv_sem=recv_sem.at[0],
        device_id=_dev(me), device_id_type=MESH).wait_send()


def _exchange(weights, owner_map):
    hbm = pl.BlockSpec(memory_space=pltpu.HBM)
    vmem = pl.BlockSpec(memory_space=pltpu.VMEM)
    return pl.pallas_call(
        _body,
        name="exchange",
        out_shape=(jax.ShapeDtypeStruct((TILES, ROWS, LANES), BF16), jax.ShapeDtypeStruct((TILES, LANES), F32)),
        in_specs=[hbm, hbm],
        out_specs=(vmem, vmem),
        scratch_shapes=[
            pltpu.VMEM((TILES, ROWS, LANES), BF16),
            pltpu.VMEM((N, 2, ROWS, LANES), BF16),
            pltpu.VMEM((N, 2, ROWS, LANES), BF16),
            pltpu.SMEM((N,), I32),
            pltpu.SMEM((1, TILES), I32),
            pltpu.VMEM((2, 8, LANES), I32),
            pltpu.SMEM((2, 8, LANES), I32),
            pltpu.VMEM((3, 8, LANES), F32),
            pltpu.VMEM((LINES, 8, LANES), F32),
            pltpu.SemaphoreType.DMA,
            pltpu.SemaphoreType.DMA,
            pltpu.SemaphoreType.DMA,
            pltpu.SemaphoreType.DMA,
            pltpu.SemaphoreType.DMA((len(CUTS) - 1,)),
            pltpu.SemaphoreType.DMA,
            pltpu.SemaphoreType.DMA((3,)),
            pltpu.SemaphoreType.REGULAR,
        ],
        compiler_params=pltpu.CompilerParams(
            collective_id=0, has_side_effects=True, vmem_limit_bytes=24 * 2**20),
    )(pltpu.with_memory_space_constraint(weights.reshape(8, ROWS, -1), pltpu.HBM), pltpu.with_memory_space_constraint(owner_map, pltpu.HBM))


def _flush_body(tiles_ref, scales_ref, out_ref, scale_ref, sem):
    copies = [pltpu.make_async_copy(scales_ref, scale_ref, sem.at[8])]
    step = TILES // 8
    for i in range(8):
        copies.append(pltpu.make_async_copy(
            tiles_ref.at[pl.ds(i * step, step)], out_ref.at[pl.ds(i * step, step)], sem.at[i]))
    for c in copies:
        c.start()
    for c in copies:
        c.wait()


def _flush(tiles, scales):
    hbm = pl.BlockSpec(memory_space=pltpu.HBM)
    vmem = pl.BlockSpec(memory_space=pltpu.VMEM)
    return pl.pallas_call(
        _flush_body,
        name="flush",
        out_shape=(jax.ShapeDtypeStruct((TILES, ROWS, LANES), BF16), jax.ShapeDtypeStruct((TILES, LANES), F32)),
        in_specs=[vmem, vmem],
        out_specs=(hbm, hbm),
        scratch_shapes=[pltpu.SemaphoreType.DMA((9,))],
        compiler_params=pltpu.CompilerParams(vmem_limit_bytes=16 * 2**20),
    )(tiles, scales)


def body(weights, owner_map):
    return _flush(*_exchange(weights, owner_map))


def solution(mesh):
    return jax.shard_map(
        body,
        mesh=mesh,
        in_specs=(P("fsdp", "tp"), P(("fsdp", "tp"), None)),
        out_specs=(P(("fsdp", "tp"), None, None), P(("fsdp", "tp"), None)),
        check_vma=False,
    )
```

```python
import random

import jax
import jax.numpy as jnp
from jax import lax
from jax.experimental import pallas as pl
from jax.experimental.pallas import tpu as pltpu
from jax.sharding import PartitionSpec as P

MESH = pl.DeviceIdType.MESH
N = 128
TILES = 256
ROWS = 32
LANES = 128
BLOCKS = 32
F32 = jnp.float32
BF16 = jnp.bfloat16
I32 = jnp.int32


def _hops(m):
    ring = (0, 1, 2, 1)
    return ring[(m >> 2) & 3] + ring[(m >> 4) & 3] + ring[(m >> 6) * 2 + ((m >> 1) & 1)]


def _plane(m):
    return (m >> 6) == 0 and ((m >> 1) & 1) == 0


PRE_CORE = 16
PRE = 40
_rng = random.Random(3)
_all = list(range(1, N))
_rng.shuffle(_all)
_all.sort(key=lambda m: -_hops(m))
NEAR = [m for m in _all if (m % 2 == 0 and (_hops(m) <= 3 or _plane(m))) or m == 1]
ORDER = [
    74, 34, 44, 66, 62, 118, 86, 80, 30, 36, 54, 24, 126, 22, 112, 98,
    11, 45, 113, 37, 63, 31, 69, 95, 119, 55, 35, 87, 75, 77, 127, 94,
    57, 99, 76, 68, 23, 25, 81, 10, 120, 106, 121, 89, 101, 109, 100, 108,
    105, 42, 107, 88, 43, 26, 92, 103, 117, 47, 116, 93, 67, 90, 96, 27,
    59, 111, 72, 84, 85, 97, 91, 124, 110, 125, 46, 58, 122, 123, 39, 102,
    71, 52, 7, 60, 21, 40, 19, 14, 73, 104, 9, 61, 79, 20, 82, 78,
    65, 50, 64, 51, 8, 6, 83, 15, 32, 18, 114, 5, 70, 115, 33, 28,
    29, 13, 3, 49, 53, 41, 12, 16, 17, 56, 48, 4, 2, 1, 38,
]
assert sorted(ORDER) == list(range(1, N))
assert all(m in NEAR and m > 1 for m in ORDER[:PRE_CORE])
assert all(m in NEAR or m - 1 in NEAR for m in ORDER[:PRE] if m > 1)
LINE_Z = [2, 64, 66]
LINE_Y = [16, 32, 48]
LINE_X = [1, 4, 5, 8, 9, 12, 13]
CUTS = list(range(0, 120, 8)) + [120, 124, 127]
LINES = len(LINE_X) + len(LINE_Y) + len(LINE_Z)


def _dev(p):
    return (lax.div(p, 4), lax.rem(p, 4))


def _body(w_hbm, map_hbm, out_ref, scale_ref, wv, sbuf, rbuf, table, map_s, pos_v, pos_s,
          peak_out, peak_in, copy_sem, map_sem, pos_sem, send_sem, recv_sem, peak_send, peak_recv, all_sem, pair_sem):
    me = lax.axis_index("fsdp") * 4 + lax.axis_index("tp")
    barrier = pltpu.get_barrier_semaphore()

    def partner(m):
        return jnp.bitwise_xor(me, m)

    def tell(sem, m):
        pl.semaphore_signal(sem, inc=1, device_id=_dev(partner(m)), device_id_type=MESH)

    map_copy = pltpu.make_async_copy(map_hbm, map_s, map_sem)
    map_copy.start()
    w_copies = []
    for c in range(BLOCKS):
        w_copies.append(pltpu.make_async_copy(
            w_hbm.at[:, :, pl.ds(c * LANES, LANES)], wv.at[pl.ds(c * 8, 8)], copy_sem))
        w_copies[-1].start()

    for m in NEAR:
        tell(barrier, m)
    for k, m in enumerate(ORDER):
        table[k] = m

    map_copy.wait()
    lane = lax.broadcasted_iota(I32, (8, LANES), 1)

    def slot(j):
        return lax.rem(j, BLOCKS) * 8 + lax.div(j, BLOCKS)

    def find(i, pos):
        low, high = pos
        for u in range(8):
            up = i * 8 + u
            down = TILES - 1 - up
            high = jnp.where(lane == map_s[0, up], slot(up), high)
            low = jnp.where(lane == map_s[0, down], slot(down), low)
        return low, high

    zero = jnp.zeros((8, LANES), I32)
    low, high = lax.fori_loop(0, TILES // 8, find, (zero, zero))
    pos_v[0:1, :] = low[0:1]
    pos_v[1:2, :] = high[0:1]
    both = pl.ds(0, 2)
    pos_copy = pltpu.make_async_copy(pos_v.at[both], pos_s.at[both], pos_sem)
    pos_copy.start()

    pltpu.make_async_copy(wv, wv, copy_sem).wait()
    pos_copy.wait()

    def gather(i, _):
        for u in range(4):
            d = i * 4 + u
            for h in range(2):
                sbuf[d, h] = wv[pos_s[h, d]]
        return 0

    lax.fori_loop(0, N // 4, gather, 0)

    def message(k, p, group):
        return pltpu.make_async_remote_copy(
            src_ref=sbuf.at[p], dst_ref=rbuf.at[k], send_sem=send_sem, recv_sem=recv_sem.at[group],
            device_id=_dev(p), device_id_type=MESH)

    def send(group):
        def one(k, _):
            message(k, partner(table[k]), group).start()
            return 0

        lax.fori_loop(CUTS[group], CUTS[group + 1], one, 0)

    def arrivals(group):
        span = pl.ds(CUTS[group], CUTS[group + 1] - CUTS[group])
        return pltpu.make_async_remote_copy(
            src_ref=sbuf.at[span], dst_ref=rbuf.at[span], send_sem=send_sem, recv_sem=recv_sem.at[group],
            device_id=_dev(me), device_id_type=MESH)

    def peaks(stage, line, base):
        copies = [pltpu.make_async_remote_copy(
            src_ref=peak_out.at[stage], dst_ref=peak_in.at[base + i],
            send_sem=peak_send, recv_sem=peak_recv.at[stage],
            device_id=_dev(partner(m)), device_id_type=MESH) for i, m in enumerate(line)]
        for c in copies:
            c.start()

    def fold(stage, line, base, value):
        span = pl.ds(base, len(line))
        pltpu.make_async_remote_copy(
            src_ref=peak_in.at[span], dst_ref=peak_in.at[span], send_sem=peak_send, recv_sem=peak_recv.at[stage],
            device_id=_dev(me), device_id_type=MESH).wait_recv()
        for i in range(len(line)):
            value = jnp.maximum(value, peak_in[base + i])
        return value

    def finish(p, pair):
        x = pair.astype(F32)
        clipped = jnp.maximum(jnp.max(jnp.abs(x), axis=1, keepdims=True), 1.0)
        out_ref[pl.ds(2 * p, 2)] = (x * (448.0 / clipped)).astype(BF16)
        scale_ref[pl.ds(2 * p, 2), :] = clipped.reshape(2, LANES)

    def receive(group):
        arrivals(group).wait_recv()

        def one(k, _):
            finish(partner(table[k]), rbuf[k])
            return 0

        lax.fori_loop(CUTS[group], CUTS[group + 1], one, 0)

    pl.semaphore_wait(barrier, len(NEAR))
    for m in LINE_Z:
        tell(all_sem, m)
    tell(pair_sem.at[0], 1)
    for g in range(PRE_CORE // 8):
        send(g)

    def largest(i, ends):
        high, low = ends
        for u in range(8):
            x = wv[i * 8 + u]
            high, low = jnp.maximum(high, x), jnp.minimum(low, x)
        return high, low

    zero = jnp.zeros((ROWS, LANES), BF16)
    high, low = lax.fori_loop(0, BLOCKS, largest, (zero, zero))
    peak = jnp.maximum(high.astype(F32), -low.astype(F32))
    peak = jnp.maximum(jnp.maximum(peak[:8], peak[8:16]), jnp.maximum(peak[16:24], peak[24:]))
    peak_out[0] = peak
    pl.semaphore_wait(pair_sem.at[0], 1)
    peaks(0, LINE_X, 0)
    for g in range(PRE_CORE // 8, PRE // 8):
        send(g)
    pl.semaphore_wait(all_sem, len(LINE_Z))
    tell(pair_sem.at[1], 1)
    pl.semaphore_wait(pair_sem.at[1], 1)
    half = max(PRE // 8, 6)
    for g in range(PRE // 8, half):
        send(g)
    peak = fold(0, LINE_X, 0, peak)
    peak_out[1] = peak
    finish(me, sbuf[me])
    peaks(1, LINE_Y, len(LINE_X))
    for g in range(half, 11):
        send(g)
    for g in range(2):
        receive(g)
    peak = fold(1, LINE_Y, len(LINE_X), peak)
    peak_out[2] = peak
    receive(2)
    peaks(2, LINE_Z, len(LINE_X) + len(LINE_Y))
    for g in range(11, len(CUTS) - 1):
        send(g)
    for g in range(3, 12):
        receive(g)
    peak = fold(2, LINE_Z, len(LINE_X) + len(LINE_Y), peak)
    top = jnp.max(peak, keepdims=True)
    for g in range(12, len(CUTS) - 1):
        receive(g)
    scale_ref[...] = scale_ref[...] / top
    every = pl.ds(0, N - 1)
    pltpu.make_async_remote_copy(
        src_ref=sbuf.at[every], dst_ref=rbuf.at[every], send_sem=send_sem, recv_sem=recv_sem.at[0],
        device_id=_dev(me), device_id_type=MESH).wait_send()
    every = pl.ds(0, LINES)
    pltpu.make_async_remote_copy(
        src_ref=peak_in.at[every], dst_ref=peak_in.at[every], send_sem=peak_send, recv_sem=recv_sem.at[0],
        device_id=_dev(me), device_id_type=MESH).wait_send()


def _exchange(weights, owner_map):
    hbm = pl.BlockSpec(memory_space=pltpu.HBM)
    vmem = pl.BlockSpec(memory_space=pltpu.VMEM)
    return pl.pallas_call(
        _body,
        name="exchange",
        out_shape=(jax.ShapeDtypeStruct((TILES, ROWS, LANES), BF16), jax.ShapeDtypeStruct((TILES, LANES), F32)),
        in_specs=[hbm, hbm],
        out_specs=(vmem, vmem),
        scratch_shapes=[
            pltpu.VMEM((TILES, ROWS, LANES), BF16),
            pltpu.VMEM((N, 2, ROWS, LANES), BF16),
            pltpu.VMEM((N, 2, ROWS, LANES), BF16),
            pltpu.SMEM((N,), I32),
            pltpu.SMEM((1, TILES), I32),
            pltpu.VMEM((8, LANES), I32),
            pltpu.SMEM((8, LANES), I32),
            pltpu.VMEM((3, 8, LANES), F32),
            pltpu.VMEM((LINES, 8, LANES), F32),
            pltpu.SemaphoreType.DMA,
            pltpu.SemaphoreType.DMA,
            pltpu.SemaphoreType.DMA,
            pltpu.SemaphoreType.DMA,
            pltpu.SemaphoreType.DMA((len(CUTS) - 1,)),
            pltpu.SemaphoreType.DMA,
            pltpu.SemaphoreType.DMA((3,)),
            pltpu.SemaphoreType.REGULAR,
            pltpu.SemaphoreType.REGULAR((2,)),
        ],
        compiler_params=pltpu.CompilerParams(
            collective_id=0, has_side_effects=True, vmem_limit_bytes=24 * 2**20),
    )(pltpu.with_memory_space_constraint(weights.reshape(8, ROWS, -1), pltpu.HBM), pltpu.with_memory_space_constraint(owner_map, pltpu.HBM))


def _flush_body(tiles_ref, scales_ref, out_ref, scale_ref, sem):
    copies = [pltpu.make_async_copy(scales_ref, scale_ref, sem.at[2])]
    step = TILES // 2
    for i in range(2):
        copies.append(pltpu.make_async_copy(
            tiles_ref.at[pl.ds(i * step, step)], out_ref.at[pl.ds(i * step, step)], sem.at[i]))
    for c in copies:
        c.start()
    for c in copies:
        c.wait()


def _flush(tiles, scales):
    hbm = pl.BlockSpec(memory_space=pltpu.HBM)
    vmem = pl.BlockSpec(memory_space=pltpu.VMEM)
    return pl.pallas_call(
        _flush_body,
        name="flush",
        out_shape=(jax.ShapeDtypeStruct((TILES, ROWS, LANES), BF16), jax.ShapeDtypeStruct((TILES, LANES), F32)),
        in_specs=[vmem, vmem],
        out_specs=(hbm, hbm),
        scratch_shapes=[pltpu.SemaphoreType.DMA((3,))],
        compiler_params=pltpu.CompilerParams(vmem_limit_bytes=16 * 2**20),
    )(tiles, scales)


def body(weights, owner_map):
    return _flush(*_exchange(weights, owner_map))


def solution(mesh):
    return jax.shard_map(
        body,
        mesh=mesh,
        in_specs=(P("fsdp", "tp"), P(("fsdp", "tp"), None)),
        out_specs=(P(("fsdp", "tp"), None, None), P(("fsdp", "tp"), None)),
        check_vma=False,
    )
```

```python
import random

import jax
import jax.numpy as jnp
from jax import lax
from jax.experimental import pallas as pl
from jax.experimental.pallas import tpu as pltpu
from jax.sharding import PartitionSpec as P

MESH = pl.DeviceIdType.MESH
N = 128
TILES = 256
ROWS = 32
LANES = 128
BLOCKS = 32
F32 = jnp.float32
BF16 = jnp.bfloat16
I32 = jnp.int32


def _hops(m):
    ring = (0, 1, 2, 1)
    return ring[(m >> 2) & 3] + ring[(m >> 4) & 3] + ring[(m >> 6) * 2 + ((m >> 1) & 1)]


def _plane(m):
    return (m >> 6) == 0 and ((m >> 1) & 1) == 0


PRE_CORE = 16
PRE = 40
_rng = random.Random(3)
_all = list(range(1, N))
_rng.shuffle(_all)
_all.sort(key=lambda m: -_hops(m))
NEAR = [m for m in _all if (m % 2 == 0 and (_hops(m) <= 3 or _plane(m))) or m == 1]
ORDER = [
    74, 34, 44, 66, 62, 118, 86, 80, 30, 36, 54, 24, 126, 22, 112, 98,
    23, 11, 45, 113, 37, 63, 31, 69, 95, 119, 55, 35, 87, 75, 77, 127,
    79, 57, 99, 76, 68, 25, 81, 10, 120, 106, 121, 89, 101, 109, 100, 108,
    105, 42, 107, 88, 43, 26, 53, 103, 123, 117, 47, 116, 93, 41, 90, 96,
    27, 59, 111, 72, 65, 85, 97, 91, 124, 125, 46, 58, 9, 39, 102, 70,
    52, 7, 60, 21, 40, 19, 14, 73, 110, 104, 122, 61, 94, 20, 82, 78,
    84, 50, 64, 51, 8, 6, 83, 15, 32, 18, 114, 92, 71, 115, 33, 28,
    29, 13, 3, 49, 5, 67, 12, 16, 17, 56, 48, 4, 2, 1, 38,
]
assert sorted(ORDER) == list(range(1, N))
assert all(m in NEAR and m > 1 for m in ORDER[:PRE_CORE])
assert all(m in NEAR or m - 1 in NEAR for m in ORDER[:PRE] if m > 1)
LINE_Z = [2, 64, 66]
LINE_Y = [16, 32, 48]
LINE_X = [1, 4, 5, 8, 9, 12, 13]
CUTS = list(range(0, 120, 8)) + [120, 124, 127]
LINES = len(LINE_X) + len(LINE_Y) + len(LINE_Z)


def _dev(p):
    return (lax.div(p, 4), lax.rem(p, 4))


def _body(w_hbm, map_hbm, out_ref, scale_ref, wv, sbuf, rbuf, table, map_s, pos_v, pos_s,
          peak_out, peak_in, copy_sem, map_sem, pos_sem, send_sem, recv_sem, peak_send, peak_recv, all_sem, pair_sem):
    me = lax.axis_index("fsdp") * 4 + lax.axis_index("tp")
    barrier = pltpu.get_barrier_semaphore()

    def partner(m):
        return jnp.bitwise_xor(me, m)

    def tell(sem, m):
        pl.semaphore_signal(sem, inc=1, device_id=_dev(partner(m)), device_id_type=MESH)

    map_copy = pltpu.make_async_copy(map_hbm, map_s, map_sem)
    map_copy.start()
    w_copies = []
    for c in range(BLOCKS):
        w_copies.append(pltpu.make_async_copy(
            w_hbm.at[:, :, pl.ds(c * LANES, LANES)], wv.at[pl.ds(c * 8, 8)], copy_sem))
        w_copies[-1].start()

    for m in NEAR:
        tell(barrier, m)
    for k, m in enumerate(ORDER):
        table[k] = m

    map_copy.wait()
    lane = lax.broadcasted_iota(I32, (8, LANES), 1)

    def slot(j):
        return lax.rem(j, BLOCKS) * 8 + lax.div(j, BLOCKS)

    def find(i, pos):
        low, high = pos
        for u in range(8):
            up = i * 8 + u
            down = TILES - 1 - up
            high = jnp.where(lane == map_s[0, up], slot(up), high)
            low = jnp.where(lane == map_s[0, down], slot(down), low)
        return low, high

    zero = jnp.zeros((8, LANES), I32)
    low, high = lax.fori_loop(0, TILES // 8, find, (zero, zero))
    pos_v[0:1, :] = low[0:1]
    pos_v[1:2, :] = high[0:1]
    both = pl.ds(0, 2)
    pos_copy = pltpu.make_async_copy(pos_v.at[both], pos_s.at[both], pos_sem)
    pos_copy.start()

    pltpu.make_async_copy(wv, wv, copy_sem).wait()
    pos_copy.wait()

    def gather(i, _):
        for u in range(4):
            d = i * 4 + u
            for h in range(2):
                sbuf[d, h] = wv[pos_s[h, d]]
        return 0

    lax.fori_loop(0, N // 4, gather, 0)

    def message(k, p, group):
        return pltpu.make_async_remote_copy(
            src_ref=sbuf.at[p], dst_ref=rbuf.at[k], send_sem=send_sem, recv_sem=recv_sem.at[group],
            device_id=_dev(p), device_id_type=MESH)

    def send(group):
        def one(k, _):
            message(k, partner(table[k]), group).start()
            return 0

        lax.fori_loop(CUTS[group], CUTS[group + 1], one, 0)

    def arrivals(group):
        span = pl.ds(CUTS[group], CUTS[group + 1] - CUTS[group])
        return pltpu.make_async_remote_copy(
            src_ref=sbuf.at[span], dst_ref=rbuf.at[span], send_sem=send_sem, recv_sem=recv_sem.at[group],
            device_id=_dev(me), device_id_type=MESH)

    def peaks(stage, line, base):
        copies = [pltpu.make_async_remote_copy(
            src_ref=peak_out.at[stage], dst_ref=peak_in.at[base + i],
            send_sem=peak_send, recv_sem=peak_recv.at[stage],
            device_id=_dev(partner(m)), device_id_type=MESH) for i, m in enumerate(line)]
        for c in copies:
            c.start()

    def fold(stage, line, base, value):
        span = pl.ds(base, len(line))
        pltpu.make_async_remote_copy(
            src_ref=peak_in.at[span], dst_ref=peak_in.at[span], send_sem=peak_send, recv_sem=peak_recv.at[stage],
            device_id=_dev(me), device_id_type=MESH).wait_recv()
        for i in range(len(line)):
            value = jnp.maximum(value, peak_in[base + i])
        return value

    def finish(p, pair):
        x = pair.astype(F32)
        clipped = jnp.maximum(jnp.max(jnp.abs(x), axis=1, keepdims=True), 1.0)
        out_ref[pl.ds(2 * p, 2)] = (x * (448.0 / clipped)).astype(BF16)
        scale_ref[pl.ds(2 * p, 2), :] = clipped.reshape(2, LANES)

    def receive(group):
        arrivals(group).wait_recv()

        def one(k, _):
            finish(partner(table[k]), rbuf[k])
            return 0

        lax.fori_loop(CUTS[group], CUTS[group + 1], one, 0)

    pl.semaphore_wait(barrier, len(NEAR))
    for m in LINE_Z:
        tell(all_sem, m)
    tell(pair_sem.at[0], 1)
    for g in range(PRE_CORE // 8):
        send(g)

    def largest(i, ends):
        high, low = ends
        for u in range(8):
            x = wv[i * 8 + u]
            high, low = jnp.maximum(high, x), jnp.minimum(low, x)
        return high, low

    zero = jnp.zeros((ROWS, LANES), BF16)
    high, low = lax.fori_loop(0, BLOCKS, largest, (zero, zero))
    peak = jnp.maximum(high.astype(F32), -low.astype(F32))
    peak = jnp.maximum(jnp.maximum(peak[:8], peak[8:16]), jnp.maximum(peak[16:24], peak[24:]))
    peak_out[0] = peak
    pl.semaphore_wait(pair_sem.at[0], 1)
    peaks(0, LINE_X, 0)
    for g in range(PRE_CORE // 8, PRE // 8):
        send(g)
    pl.semaphore_wait(all_sem, len(LINE_Z))
    tell(pair_sem.at[1], 1)
    pl.semaphore_wait(pair_sem.at[1], 1)
    half = max(PRE // 8, 6)
    for g in range(PRE // 8, half):
        send(g)
    peak = fold(0, LINE_X, 0, peak)
    peak_out[1] = peak
    finish(me, sbuf[me])
    peaks(1, LINE_Y, len(LINE_X))
    for g in range(half, 11):
        send(g)
    for g in range(2):
        receive(g)
    peak = fold(1, LINE_Y, len(LINE_X), peak)
    peak_out[2] = peak
    receive(2)
    peaks(2, LINE_Z, len(LINE_X) + len(LINE_Y))
    for g in range(11, len(CUTS) - 1):
        send(g)
    for g in range(3, 12):
        receive(g)
    peak = fold(2, LINE_Z, len(LINE_X) + len(LINE_Y), peak)
    top = jnp.max(peak, keepdims=True)
    for g in range(12, len(CUTS) - 1):
        receive(g)
    scale_ref[...] = scale_ref[...] / top
    every = pl.ds(0, N - 1)
    pltpu.make_async_remote_copy(
        src_ref=sbuf.at[every], dst_ref=rbuf.at[every], send_sem=send_sem, recv_sem=recv_sem.at[0],
        device_id=_dev(me), device_id_type=MESH).wait_send()
    every = pl.ds(0, LINES)
    pltpu.make_async_remote_copy(
        src_ref=peak_in.at[every], dst_ref=peak_in.at[every], send_sem=peak_send, recv_sem=recv_sem.at[0],
        device_id=_dev(me), device_id_type=MESH).wait_send()


def _exchange(weights, owner_map):
    hbm = pl.BlockSpec(memory_space=pltpu.HBM)
    vmem = pl.BlockSpec(memory_space=pltpu.VMEM)
    return pl.pallas_call(
        _body,
        name="exchange",
        out_shape=(jax.ShapeDtypeStruct((TILES, ROWS, LANES), BF16), jax.ShapeDtypeStruct((TILES, LANES), F32)),
        in_specs=[hbm, hbm],
        out_specs=(vmem, vmem),
        scratch_shapes=[
            pltpu.VMEM((TILES, ROWS, LANES), BF16),
            pltpu.VMEM((N, 2, ROWS, LANES), BF16),
            pltpu.VMEM((N, 2, ROWS, LANES), BF16),
            pltpu.SMEM((N,), I32),
            pltpu.SMEM((1, TILES), I32),
            pltpu.VMEM((8, LANES), I32),
            pltpu.SMEM((8, LANES), I32),
            pltpu.VMEM((3, 8, LANES), F32),
            pltpu.VMEM((LINES, 8, LANES), F32),
            pltpu.SemaphoreType.DMA,
            pltpu.SemaphoreType.DMA,
            pltpu.SemaphoreType.DMA,
            pltpu.SemaphoreType.DMA,
            pltpu.SemaphoreType.DMA((len(CUTS) - 1,)),
            pltpu.SemaphoreType.DMA,
            pltpu.SemaphoreType.DMA((3,)),
            pltpu.SemaphoreType.REGULAR,
            pltpu.SemaphoreType.REGULAR((2,)),
        ],
        compiler_params=pltpu.CompilerParams(
            collective_id=0, has_side_effects=True, vmem_limit_bytes=24 * 2**20),
    )(pltpu.with_memory_space_constraint(weights.reshape(8, ROWS, -1), pltpu.HBM), pltpu.with_memory_space_constraint(owner_map, pltpu.HBM))


def _flush_body(tiles_ref, scales_ref, out_ref, scale_ref, sem):
    copies = [pltpu.make_async_copy(scales_ref, scale_ref, sem.at[2])]
    step = TILES // 2
    for i in range(2):
        copies.append(pltpu.make_async_copy(
            tiles_ref.at[pl.ds(i * step, step)], out_ref.at[pl.ds(i * step, step)], sem.at[i]))
    for c in copies:
        c.start()
    for c in copies:
        c.wait()


def _flush(tiles, scales):
    hbm = pl.BlockSpec(memory_space=pltpu.HBM)
    vmem = pl.BlockSpec(memory_space=pltpu.VMEM)
    return pl.pallas_call(
        _flush_body,
        name="flush",
        out_shape=(jax.ShapeDtypeStruct((TILES, ROWS, LANES), BF16), jax.ShapeDtypeStruct((TILES, LANES), F32)),
        in_specs=[vmem, vmem],
        out_specs=(hbm, hbm),
        scratch_shapes=[pltpu.SemaphoreType.DMA((3,))],
        compiler_params=pltpu.CompilerParams(vmem_limit_bytes=16 * 2**20),
    )(tiles, scales)


def body(weights, owner_map):
    return _flush(*_exchange(weights, owner_map))


def solution(mesh):
    return jax.shard_map(
        body,
        mesh=mesh,
        in_specs=(P("fsdp", "tp"), P(("fsdp", "tp"), None)),
        out_specs=(P(("fsdp", "tp"), None, None), P(("fsdp", "tp"), None)),
        check_vma=False,
    )
```

```python
import random

import jax
import jax.numpy as jnp
from jax import lax
from jax.experimental import pallas as pl
from jax.experimental.pallas import tpu as pltpu
from jax.sharding import PartitionSpec as P

MESH = pl.DeviceIdType.MESH
N = 128
TILES = 256
ROWS = 32
LANES = 128
BLOCKS = 32
F32 = jnp.float32
BF16 = jnp.bfloat16
I32 = jnp.int32


def _hops(m):
    ring = (0, 1, 2, 1)
    return ring[(m >> 2) & 3] + ring[(m >> 4) & 3] + ring[(m >> 6) * 2 + ((m >> 1) & 1)]


def _plane(m):
    return (m >> 6) == 0 and ((m >> 1) & 1) == 0


PRE_CORE = 16
PRE = 40
_rng = random.Random(3)
_all = list(range(1, N))
_rng.shuffle(_all)
_all.sort(key=lambda m: -_hops(m))
NEAR = [m for m in _all if (m % 2 == 0 and (_hops(m) <= 3 or _plane(m))) or m == 1]
ORDER = [
    74, 34, 44, 66, 62, 118, 86, 24, 80, 30, 36, 54, 126, 22, 112, 98,
    23, 11, 45, 113, 37, 63, 31, 69, 95, 119, 55, 35, 87, 75, 77, 127,
    79, 57, 99, 76, 68, 25, 81, 10, 120, 106, 121, 89, 101, 109, 100, 108,
    105, 42, 107, 88, 43, 26, 53, 103, 123, 117, 47, 116, 93, 41, 90, 96,
    27, 59, 111, 72, 65, 85, 97, 91, 124, 125, 46, 58, 122, 39, 102, 70,
    52, 7, 60, 21, 17, 19, 14, 73, 110, 104, 9, 61, 94, 20, 82, 78,
    84, 50, 64, 51, 8, 6, 83, 15, 12, 18, 114, 92, 71, 115, 33, 28,
    29, 13, 3, 49, 5, 67, 32, 16, 40, 56, 48, 4, 2, 1, 38,
]
assert sorted(ORDER) == list(range(1, N))
assert all(m in NEAR and m > 1 for m in ORDER[:PRE_CORE])
assert all(m in NEAR or m - 1 in NEAR for m in ORDER[:PRE] if m > 1)
LINE_Z = [2, 64, 66]
LINE_Y = [16, 32, 48]
LINE_X = [1, 4, 5, 8, 9, 12, 13]
CUTS = list(range(0, 120, 8)) + [120, 124, 127]
LINES = len(LINE_X) + len(LINE_Y) + len(LINE_Z)


def _dev(p):
    return (lax.div(p, 4), lax.rem(p, 4))


def _body(w_hbm, map_hbm, out_ref, scale_ref, wv, sbuf, rbuf, table, map_s, pos_v, pos_s,
          peak_out, peak_in, copy_sem, map_sem, pos_sem, send_sem, recv_sem, peak_send, peak_recv, all_sem, pair_sem):
    me = lax.axis_index("fsdp") * 4 + lax.axis_index("tp")
    barrier = pltpu.get_barrier_semaphore()

    def partner(m):
        return jnp.bitwise_xor(me, m)

    def tell(sem, m):
        pl.semaphore_signal(sem, inc=1, device_id=_dev(partner(m)), device_id_type=MESH)

    map_copy = pltpu.make_async_copy(map_hbm, map_s, map_sem)
    map_copy.start()
    w_copies = []
    for c in range(BLOCKS):
        w_copies.append(pltpu.make_async_copy(
            w_hbm.at[:, :, pl.ds(c * LANES, LANES)], wv.at[pl.ds(c * 8, 8)], copy_sem))
        w_copies[-1].start()

    for m in NEAR:
        tell(barrier, m)
    for k, m in enumerate(ORDER):
        table[k] = m

    map_copy.wait()
    lane = lax.broadcasted_iota(I32, (8, LANES), 1)

    def slot(j):
        return lax.rem(j, BLOCKS) * 8 + lax.div(j, BLOCKS)

    def find(i, pos):
        low, high = pos
        for u in range(8):
            up = i * 8 + u
            down = TILES - 1 - up
            high = jnp.where(lane == map_s[0, up], slot(up), high)
            low = jnp.where(lane == map_s[0, down], slot(down), low)
        return low, high

    zero = jnp.zeros((8, LANES), I32)
    low, high = lax.fori_loop(0, TILES // 8, find, (zero, zero))
    pos_v[0:1, :] = low[0:1]
    pos_v[1:2, :] = high[0:1]
    both = pl.ds(0, 2)
    pos_copy = pltpu.make_async_copy(pos_v.at[both], pos_s.at[both], pos_sem)
    pos_copy.start()

    pltpu.make_async_copy(wv, wv, copy_sem).wait()
    pos_copy.wait()

    def gather(i, _):
        for u in range(4):
            d = i * 4 + u
            for h in range(2):
                sbuf[d, h] = wv[pos_s[h, d]]
        return 0

    lax.fori_loop(0, N // 4, gather, 0)

    def message(k, p, group):
        return pltpu.make_async_remote_copy(
            src_ref=sbuf.at[p], dst_ref=rbuf.at[k], send_sem=send_sem, recv_sem=recv_sem.at[group],
            device_id=_dev(p), device_id_type=MESH)

    def send(group):
        def one(k, _):
            message(k, partner(table[k]), group).start()
            return 0

        lax.fori_loop(CUTS[group], CUTS[group + 1], one, 0)

    def arrivals(group):
        span = pl.ds(CUTS[group], CUTS[group + 1] - CUTS[group])
        return pltpu.make_async_remote_copy(
            src_ref=sbuf.at[span], dst_ref=rbuf.at[span], send_sem=send_sem, recv_sem=recv_sem.at[group],
            device_id=_dev(me), device_id_type=MESH)

    def peaks(stage, line, base):
        copies = [pltpu.make_async_remote_copy(
            src_ref=peak_out.at[stage], dst_ref=peak_in.at[base + i],
            send_sem=peak_send, recv_sem=peak_recv.at[stage],
            device_id=_dev(partner(m)), device_id_type=MESH) for i, m in enumerate(line)]
        for c in copies:
            c.start()

    def fold(stage, line, base, value):
        span = pl.ds(base, len(line))
        pltpu.make_async_remote_copy(
            src_ref=peak_in.at[span], dst_ref=peak_in.at[span], send_sem=peak_send, recv_sem=peak_recv.at[stage],
            device_id=_dev(me), device_id_type=MESH).wait_recv()
        for i in range(len(line)):
            value = jnp.maximum(value, peak_in[base + i])
        return value

    def finish(p, pair):
        x = pair.astype(F32)
        clipped = jnp.maximum(jnp.max(jnp.abs(x), axis=1, keepdims=True), 1.0)
        out_ref[pl.ds(2 * p, 2)] = (x * (448.0 / clipped)).astype(BF16)
        scale_ref[pl.ds(2 * p, 2), :] = clipped.reshape(2, LANES)

    def receive(group):
        arrivals(group).wait_recv()

        def one(k, _):
            finish(partner(table[k]), rbuf[k])
            return 0

        lax.fori_loop(CUTS[group], CUTS[group + 1], one, 0)

    pl.semaphore_wait(barrier, len(NEAR))
    for m in LINE_Z:
        tell(all_sem, m)
    tell(pair_sem.at[0], 1)
    for g in range(PRE_CORE // 8):
        send(g)

    def largest(i, ends):
        high, low = ends
        for u in range(8):
            x = wv[i * 8 + u]
            high, low = jnp.maximum(high, x), jnp.minimum(low, x)
        return high, low

    zero = jnp.zeros((ROWS, LANES), BF16)
    high, low = lax.fori_loop(0, BLOCKS, largest, (zero, zero))
    peak = jnp.maximum(high.astype(F32), -low.astype(F32))
    peak = jnp.maximum(jnp.maximum(peak[:8], peak[8:16]), jnp.maximum(peak[16:24], peak[24:]))
    peak_out[0] = peak
    pl.semaphore_wait(pair_sem.at[0], 1)
    peaks(0, LINE_X, 0)
    for g in range(PRE_CORE // 8, PRE // 8):
        send(g)
    pl.semaphore_wait(all_sem, len(LINE_Z))
    tell(pair_sem.at[1], 1)
    pl.semaphore_wait(pair_sem.at[1], 1)
    half = max(PRE // 8, 6)
    for g in range(PRE // 8, half):
        send(g)
    peak = fold(0, LINE_X, 0, peak)
    peak_out[1] = peak
    finish(me, sbuf[me])
    peaks(1, LINE_Y, len(LINE_X))
    for g in range(half, 11):
        send(g)
    for g in range(2):
        receive(g)
    peak = fold(1, LINE_Y, len(LINE_X), peak)
    peak_out[2] = peak
    receive(2)
    peaks(2, LINE_Z, len(LINE_X) + len(LINE_Y))
    for g in range(11, len(CUTS) - 1):
        send(g)
    for g in range(3, 12):
        receive(g)
    peak = fold(2, LINE_Z, len(LINE_X) + len(LINE_Y), peak)
    top = jnp.max(peak, keepdims=True)
    for g in range(12, len(CUTS) - 1):
        receive(g)
    scale_ref[...] = scale_ref[...] / top
    every = pl.ds(0, N - 1)
    pltpu.make_async_remote_copy(
        src_ref=sbuf.at[every], dst_ref=rbuf.at[every], send_sem=send_sem, recv_sem=recv_sem.at[0],
        device_id=_dev(me), device_id_type=MESH).wait_send()
    every = pl.ds(0, LINES)
    pltpu.make_async_remote_copy(
        src_ref=peak_in.at[every], dst_ref=peak_in.at[every], send_sem=peak_send, recv_sem=recv_sem.at[0],
        device_id=_dev(me), device_id_type=MESH).wait_send()


def _exchange(weights, owner_map):
    hbm = pl.BlockSpec(memory_space=pltpu.HBM)
    vmem = pl.BlockSpec(memory_space=pltpu.VMEM)
    return pl.pallas_call(
        _body,
        name="exchange",
        out_shape=(jax.ShapeDtypeStruct((TILES, ROWS, LANES), BF16), jax.ShapeDtypeStruct((TILES, LANES), F32)),
        in_specs=[hbm, hbm],
        out_specs=(vmem, vmem),
        scratch_shapes=[
            pltpu.VMEM((TILES, ROWS, LANES), BF16),
            pltpu.VMEM((N, 2, ROWS, LANES), BF16),
            pltpu.VMEM((N, 2, ROWS, LANES), BF16),
            pltpu.SMEM((N,), I32),
            pltpu.SMEM((1, TILES), I32),
            pltpu.VMEM((8, LANES), I32),
            pltpu.SMEM((8, LANES), I32),
            pltpu.VMEM((3, 8, LANES), F32),
            pltpu.VMEM((LINES, 8, LANES), F32),
            pltpu.SemaphoreType.DMA,
            pltpu.SemaphoreType.DMA,
            pltpu.SemaphoreType.DMA,
            pltpu.SemaphoreType.DMA,
            pltpu.SemaphoreType.DMA((len(CUTS) - 1,)),
            pltpu.SemaphoreType.DMA,
            pltpu.SemaphoreType.DMA((3,)),
            pltpu.SemaphoreType.REGULAR,
            pltpu.SemaphoreType.REGULAR((2,)),
        ],
        compiler_params=pltpu.CompilerParams(
            collective_id=0, has_side_effects=True, vmem_limit_bytes=24 * 2**20),
    )(pltpu.with_memory_space_constraint(weights.reshape(8, ROWS, -1), pltpu.HBM), pltpu.with_memory_space_constraint(owner_map, pltpu.HBM))


def _flush_body(tiles_ref, scales_ref, out_ref, scale_ref, sem):
    copies = [
        pltpu.make_async_copy(tiles_ref, out_ref, sem.at[0]),
        pltpu.make_async_copy(scales_ref, scale_ref, sem.at[1]),
    ]
    for c in copies:
        c.start()
    for c in copies:
        c.wait()


def _flush(tiles, scales):
    hbm = pl.BlockSpec(memory_space=pltpu.HBM)
    vmem = pl.BlockSpec(memory_space=pltpu.VMEM)
    return pl.pallas_call(
        _flush_body,
        name="flush",
        out_shape=(jax.ShapeDtypeStruct((TILES, ROWS, LANES), BF16), jax.ShapeDtypeStruct((TILES, LANES), F32)),
        in_specs=[vmem, vmem],
        out_specs=(hbm, hbm),
        scratch_shapes=[pltpu.SemaphoreType.DMA((2,))],
        compiler_params=pltpu.CompilerParams(vmem_limit_bytes=16 * 2**20),
    )(tiles, scales)


def body(weights, owner_map):
    return _flush(*_exchange(weights, owner_map))


def solution(mesh):
    return jax.shard_map(
        body,
        mesh=mesh,
        in_specs=(P("fsdp", "tp"), P(("fsdp", "tp"), None)),
        out_specs=(P(("fsdp", "tp"), None, None), P(("fsdp", "tp"), None)),
        check_vma=False,
    )
```
